32 devices in a mesh: gx: 4 (over x, core), gy: 4 (over z), gz: 2 (over y).
Axes of the slice: x: 2, y: 2, z: 4, core: 2. Of those that a mesh axis runs over, the one named last changes fastest.
Arguments:
- occupied: float32 [16, 16, 16, 256], P(None, 'gx', 'gy', 'gz'), may hold values from -6 to 6
- virtual: float32 [16, 16, 16, 256], P(None, 'gx', 'gy', 'gz'), may hold values from -6 to 6
- kernel_fields: float32 [4, 16, 16, 256], P(None, 'gx', 'gy', 'gz'), may hold values from -1.5 to 1.5
- density_grad: float32 [3, 16, 16, 256], P(None, 'gx', 'gy', 'gz'), may hold values from -6 to 6
Outputs:
- potential: float32 [256, 16, 16, 256], P(None, 'gx', 'gy', 'gz')
- casida: float32 [256, 256], P(('gx', 'gy', 'gz'))
The draws below stay inside these ranges and needn't reach their ends.
All inputs are finite; a program needn't handle non-finite values.
Results may differ from the reference program's by a relative error of at most 0.00013.
Values sent between devices are 32-bit elements; how exact they have to be, the bound alone decides.
A program may use at most 64 MiB of HBM per device.

```python
import jax
import jax.numpy as jnp
from jax import lax

NOCC = 16
NVIR = 16
NX = 16
NY = 16
NZ = 256


def steps_of(rng, extent, split, low, high):
    loudness = 1.0
    for axis_at, blocks in split:
        steps = jax.random.uniform(jax.random.fold_in(jax.random.fold_in(rng, 6), axis_at), (blocks,), jnp.float32, low / len(split), high / len(split))
        loudness = loudness * jnp.repeat(jnp.exp(steps), extent[axis_at] // blocks).reshape((-1,) + (1,) * (len(extent) - 1 - axis_at))
    return loudness


def scatter_about(own_key, extent, scale, most, split=(), held_as=jnp.bfloat16):
    gain = steps_of(own_key, extent, split, -0.22, 0.18) if split else 1.0
    array = jax.random.normal(own_key, extent, jnp.float32) * scale * gain
    return jnp.minimum(jnp.maximum(array, -most), most).astype(held_as)


def setup_inputs(seed: int = 0) -> dict:
    keys = jax.random.split(jax.random.key(seed), 5)
    occupied = scatter_about(keys[0], (NOCC, NX, NY, NZ), 1.0, 6.0, ((1, 4), (2, 4), (3, 2)), jnp.float32)
    virtual = scatter_about(keys[1], (NVIR, NX, NY, NZ), 1.0, 6.0, ((1, 4), (2, 4), (3, 2)), jnp.float32)
    kernel_fields = jnp.clip(jax.random.uniform(keys[2], (4, NX, NY, NZ), jnp.float32, -1.5, 1.5) * steps_of(keys[2], (4, NX, NY, NZ), ((1, 4), (2, 4), (3, 2)), -0.4, 0.0), -1.5, 1.5)
    density_grad = scatter_about(keys[3], (3, NX, NY, NZ), 1.0, 6.0, ((1, 4), (2, 4), (3, 2)), jnp.float32)
    return {"occupied": occupied, "virtual": virtual, "kernel_fields": kernel_fields, "density_grad": density_grad}


def derivative(values, dimension):
    inner_diff = jnp.roll(values, -1, dimension) - jnp.roll(values, 1, dimension)
    outer_diff = jnp.roll(values, -2, dimension) - jnp.roll(values, 2, dimension)
    return (8.0 * inner_diff - outer_diff) / 12.0


def respond(densities, kernel_fields, density_grad):
    slopes = [derivative(densities, dimension + 1) for dimension in range(3)]
    aligned = density_grad[0] * slopes[0] + density_grad[1] * slopes[1] + density_grad[2] * slopes[2]
    scalar = kernel_fields[1] * densities + kernel_fields[2] * aligned
    fluxes = [scalar * density_grad[dimension] + kernel_fields[3] * slopes[dimension] for dimension in range(3)]
    divergence = derivative(fluxes[0], 1) + derivative(fluxes[1], 2) + derivative(fluxes[2], 3)
    return kernel_fields[0] * densities + kernel_fields[1] * aligned - divergence


def reference(occupied, virtual, kernel_fields, density_grad):
    def pair_block(orbital):
        return respond(orbital[None] * virtual, kernel_fields, density_grad)

    potential = lax.map(pair_block, occupied).reshape((NOCC * NVIR, NX, NY, NZ))
    flat_potential = potential.reshape((NOCC * NVIR, NX * NY * NZ))

    def rows_of(orbital):
        densities = (orbital[None] * virtual).reshape((NVIR, NX * NY * NZ))
        return lax.dot_general(densities, flat_potential, (((1,), (1,)), ((), ())), precision=lax.Precision.HIGHEST, preferred_element_type=jnp.float32)

    casida = lax.map(rows_of, occupied).reshape((NOCC * NVIR, NOCC * NVIR)) * (1.0 / (NX * NY * NZ))
    return potential, casida
```

```python
import functools

import jax
import jax.numpy as jnp
from jax import lax
from jax.experimental import pallas as pl
from jax.experimental.pallas import tpu as pltpu
from jax.sharding import PartitionSpec as P

MESH = pl.DeviceIdType.MESH
F32 = jnp.float32
BF16 = jnp.bfloat16


def halo_kernel(orb, fld, zed, zfl, arms, corners, fx, fy, zz, zg, zx, zy, send, recv):
    nx, ny, nz = (lax.axis_size(a) for a in ("gx", "gy", "gz"))
    x, y, z = (lax.axis_index(a) for a in ("gx", "gy", "gz"))
    bx, by = orb.shape[0], orb.shape[1]
    up = lambda v, n: lax.rem(v + 1, n)
    dn = lambda v, n: lax.rem(v + n - 1, n)
    xs = (dn(x, nx), up(x, nx))
    ys = (dn(y, ny), up(y, ny))
    zs = (dn(z, nz), up(z, nz))

    def dev(gx=None, gy=None, gz=None):
        return {
            "gx": x if gx is None else gx,
            "gy": y if gy is None else gy,
            "gz": z if gz is None else gz,
        }

    barrier = pltpu.get_barrier_semaphore()
    others = [dev(gx=v) for v in xs] + [dev(gy=v) for v in ys] + [dev(gz=v) for v in zs]
    others += [dev(gx=v, gy=w) for v in xs for w in ys]
    for d in others:
        pl.semaphore_signal(barrier, inc=1, device_id=d, device_id_type=MESH)
    pl.semaphore_wait(barrier, len(others))

    copies = []

    def put(src, dst, device):
        k = len(copies)
        c = pltpu.make_async_remote_copy(
            src_ref=src,
            dst_ref=dst,
            send_sem=send.at[k],
            recv_sem=recv.at[k],
            device_id=device,
            device_id_type=MESH,
        )
        c.start()
        copies.append(c)

    for side in range(2):
        put(zed, zz.at[side], dev(gz=zs[1 - side]))
        put(zfl, zg.at[side], dev(gz=zs[1 - side]))
    first_z = list(copies)
    for side in range(2):
        lo_x = pl.ds(bx - 2, 2) if side == 0 else pl.ds(0, 2)
        lo_y = pl.ds(by - 2, 2) if side == 0 else pl.ds(0, 2)
        put(orb, arms.at[side], dev(gx=xs[1 - side]))
        put(orb, arms.at[2 + side], dev(gy=ys[1 - side]))
        put(fld.at[lo_x], fx.at[side], dev(gx=xs[1 - side]))
        put(fld.at[:, lo_y], fy.at[side], dev(gy=ys[1 - side]))
    for sx in range(2):
        for sy in range(2):
            lo_x = pl.ds(bx - 2, 2) if sx == 0 else pl.ds(0, 2)
            lo_y = pl.ds(by - 2, 2) if sy == 0 else pl.ds(0, 2)
            put(
                orb.at[lo_x, lo_y],
                corners.at[2 * sx + sy],
                dev(gx=xs[1 - sx], gy=ys[1 - sy]),
            )
    for c in first_z:
        c.wait()
    for side in range(2):
        lo_x = pl.ds(bx - 2, 2) if side == 0 else pl.ds(0, 2)
        lo_y = pl.ds(by - 2, 2) if side == 0 else pl.ds(0, 2)
        for zside in range(2):
            put(zz.at[zside, lo_x], zx.at[side, zside], dev(gx=xs[1 - side]))
            put(zz.at[zside, :, lo_y], zy.at[side, zside], dev(gy=ys[1 - side]))
    for c in copies[len(first_z):]:
        c.wait()


def main_kernel(
    norb, orb, fld, k0, arms, corners, fx, fy, zz, zg, zx, zy,
    pot, part,
    nS, oS, vS, vE, eF, C, A0, A1, f0, f1, f2, base, ph, plo, nh, nl,
):
    nocc, nvir = norb
    bx, by = orb.shape[0], orb.shape[1]
    lanes = orb.shape[3]
    i = pl.program_id(0)
    shifts = (1, -1, 2, -2)

    def src(x, y):
        inx, iny = 0 <= x < bx, 0 <= y < by
        if inx and iny:
            return orb.at[x, y]
        if iny:
            return arms.at[0, x + bx, y] if x < 0 else arms.at[1, x - bx, y]
        if inx:
            return arms.at[2, x, y + by] if y < 0 else arms.at[3, x, y - by]
        sx, sy = int(x >= 0), int(y >= 0)
        return corners.at[2 * sx + sy, x - bx if sx else x + 2, y - by if sy else y + 2]

    def zsrc(x, y, zside):
        inx, iny = 0 <= x < bx, 0 <= y < by
        if inx and iny:
            return zz.at[zside, x, y]
        if iny:
            return zx.at[0, zside, x + 2, y] if x < 0 else zx.at[1, zside, x - bx, y]
        return zy.at[0, zside, x, y + 2] if y < 0 else zy.at[1, zside, x, y - by]

    def fsrc(x, y):
        inx, iny = 0 <= x < bx, 0 <= y < by
        if inx and iny:
            return fld.at[x, y]
        if iny:
            return fx.at[0, x + 2, y] if x < 0 else fx.at[1, x - bx, y]
        return fy.at[0, x, y + 2] if y < 0 else fy.at[1, x, y - by]

    center = [(x, y) for x in range(bx) for y in range(by)]
    xarm = [(x, y) for x in (-2, -1, bx, bx + 1) for y in range(by)]
    yarm = [(x, y) for x in range(bx) for y in (-2, -1, by, by + 1)]
    near = center + xarm + yarm
    far = [(x, y) for x in (-4, -3, bx + 2, bx + 3) for y in range(by)]
    far += [(x, y) for x in range(bx) for y in (-4, -3, by + 2, by + 3)]
    far += [(x, y) for x in (-2, -1, bx, bx + 1) for y in (-2, -1, by, by + 1)]
    lane = lax.broadcasted_iota(jnp.int32, (nvir, lanes), 1)

    def slope(f):
        return 8.0 * (f(1) - f(-1)) - (f(2) - f(-2))

    @pl.when(i == 0)
    def _():
        lane1 = lax.broadcasted_iota(jnp.int32, (1, lanes), 1)
        upper = (lane1 & 7) < 4
        edge = (lane < 2) | (lane >= lanes - 2)

        row = lax.broadcasted_iota(jnp.int32, (nocc, lanes), 0)
        owner = lax.rem(((lane + 2) // 8) + row, lanes // 8) == 0

        def wrapped(s):
            return lane < s if s > 0 else lane >= lanes + s

        def spread(v):
            v = jnp.where(edge, v, 0.0)
            step = 8
            while step < lanes:
                v = v + pltpu.roll(v, step, 1)
                step *= 2
            return v

        for x, y in near:
            rows = jnp.where(upper, zsrc(x, y, 1)[...], zsrc(x, y, 0)[...])
            o_alt = pltpu.roll(
                jnp.broadcast_to(rows[0:1], (nocc, lanes)), 0, 1, stride=8, stride_axis=0
            )
            v_alt = pltpu.roll(
                jnp.broadcast_to(rows[1:2], (nvir, lanes)), 0, 1, stride=8, stride_axis=0
            )
            o_own = src(x, y)[0:nocc]
            v_own = src(x, y)[nocc:nocc + nvir]
            eS_v = spread(v_alt)
            vE[0, x + 2, y + 2] = rows[0:1] * eS_v
            middle = 0 <= x < bx and 0 <= y < by
            for k, s in enumerate(shifts):
                m = wrapped(s)
                roll = (-s) % lanes
                scale = 8.0 if abs(s) == 1 else 1.0
                oS[k, x + 2, y + 2] = scale * pltpu.roll(jnp.where(m, o_alt, o_own), roll, 1)
                vS[k, x + 2, y + 2] = pltpu.roll(jnp.where(m, v_alt, v_own), roll, 1)
                if middle:
                    oe = scale * pltpu.roll(jnp.where(m, o_own, o_alt), roll, 1)
                    ve = pltpu.roll(jnp.where(m, v_own, v_alt), roll, 1)
                    oe = jnp.where(owner, spread(oe), 0.0)
                    oe = jnp.sum(oe, axis=0, keepdims=True)
                    vE[1 + k, x + 2, y + 2] = oe * spread(ve)

        for x, y in center:
            g = jnp.where(upper, zg[1, x, y], zg[0, x, y])
            g0, g1, g2 = g[0:1], g[1:2], g[2:3]
            k1, k2, k3 = g[3:4], g[4:5], g[5:6]
            at = lambda dx, dy: vE[0, x + 2 + dx, y + 2 + dy]
            s0 = slope(lambda t: at(t, 0))
            s1 = slope(lambda t: at(0, t))
            s2 = (vE[1, x + 2, y + 2] - vE[2, x + 2, y + 2]) - (
                vE[3, x + 2, y + 2] - vE[4, x + 2, y + 2]
            )
            eF[x, y] = (
                (k2 * g2 * g0) * s0
                + (k2 * g2 * g1) * s1
                + (k2 * g2 * g2 + k3) * s2
                + (k1 * g2) * at(0, 0)
            )
        for x, y in center:
            f = fsrc(x, y)[...]
            for k in range(6):
                C[k, x, y] = jnp.broadcast_to(f[k:k + 1], (8, lanes))
            C[6, x, y] = jnp.broadcast_to(k0[x, y], (8, lanes))
        for arm, cells, me in ((A0, xarm, 0), (A1, yarm, 1)):
            for at, (x, y) in enumerate(cells):
                f = fsrc(x, y)[...]
                gm = f[me:me + 1]
                for k in range(3):
                    c = f[4:5] * gm * f[k:k + 1]
                    if k == me:
                        c = c + f[5:6]
                    arm[k, at] = jnp.broadcast_to(c, (8, lanes))
                arm[3, at] = jnp.broadcast_to(f[3:4] * gm, (8, lanes))

    def rows2(c):
        return jnp.concatenate([c] * (nvir // 8), axis=0)

    off = 4
    for x, y in near + far:
        cell = src(x, y)
        nS[x + off, y + off] = cell[pl.ds(i, 1)] * cell[nocc:nocc + nvir]

    def n_at(x, y):
        return nS[x + off, y + off]

    def slopes(x, y):
        s0 = slope(lambda t: n_at(x + t, y))
        s1 = slope(lambda t: n_at(x, y + t))
        p = [oS[k, x + 2, y + 2, pl.ds(i, 1)] * vS[k, x + 2, y + 2] for k in range(4)]
        return s0, s1, (p[0] - p[1]) - (p[2] - p[3])

    for arm, cells, out in ((A0, xarm, f0), (A1, yarm, f1)):
        for at, (x, y) in enumerate(cells):
            s0, s1, s2 = slopes(x, y)
            value = (
                rows2(arm[0, at]) * s0
                + rows2(arm[1, at]) * s1
                + rows2(arm[2, at]) * s2
                + rows2(arm[3, at]) * n_at(x, y)
            )
            if out is f0:
                f0[x + 2, y] = value
            else:
                f1[x, y + 2] = value

    back = 8 * i
    row0 = pl.multiple_of(i * nvir, nvir)
    for x, y in center:
        s0, s1, s2 = slopes(x, y)
        g0, g1, g2, k1, k2, k3, kk = (rows2(C[k, x, y]) for k in range(7))
        n = n_at(x, y)
        al = g0 * s0 + g1 * s1 + g2 * s2
        sc = k1 * n + k2 * al
        f0[x + 2, y] = sc * g0 + k3 * s0
        f1[x, y + 2] = sc * g1 + k3 * s1
        f = sc * g2 + k3 * s2
        e = pltpu.roll(eF[x, y], back, 1)
        up1 = pltpu.roll(jnp.where(lane < 1, e, f), lanes - 1, 1)
        up2 = pltpu.roll(jnp.where(lane < 2, e, f), lanes - 2, 1)
        dn1 = pltpu.roll(jnp.where(lane >= lanes - 1, e, f), 1, 1)
        dn2 = pltpu.roll(jnp.where(lane >= lanes - 2, e, f), 2, 1)
        base[x, y] = kk * n + k1 * al - (8.0 * (up1 - dn1) - (up2 - dn2))
        at = (x * by + y) * lanes
        hi = n.astype(BF16)
        nh[pl.ds(row0, nvir), at:at + lanes] = hi
        nl[pl.ds(row0, nvir), at:at + lanes] = (n - hi.astype(F32)).astype(BF16)

    for x, y in center:
        inner = (f0[x + 3, y] - f0[x + 1, y]) + (f1[x, y + 3] - f1[x, y + 1])
        outer = (f0[x + 4, y] - f0[x, y]) + (f1[x, y + 4] - f1[x, y])
        v = base[x, y] - (8.0 * inner - outer)
        cell = x * by + y
        pot[pl.ds(cell, nvir, stride=bx * by), :] = v
        at = cell * lanes
        hi = v.astype(BF16)
        ph[pl.ds(row0, nvir), at:at + lanes] = hi
        plo[pl.ds(row0, nvir), at:at + lanes] = (v - hi.astype(F32)).astype(BF16)

    @pl.when(i == nocc - 1)
    def _():
        def dot(a, b):
            return lax.dot_general(
                a[...], b[...], (((1,), (1,)), ((), ())), preferred_element_type=F32
            )

        part[...] = dot(nh, ph) + dot(nh, plo) + dot(nl, ph)


def scatter_kernel(scale, part, out, got, send, recv):
    nx, ny, nz = (lax.axis_size(a) for a in ("gx", "gy", "gz"))
    n = nx * ny * nz
    me = (lax.axis_index("gx") * ny + lax.axis_index("gy")) * nz + lax.axis_index("gz")

    def dev(d):
        t = lax.rem(me + d, n)
        return t, {"gx": t // (ny * nz), "gy": lax.rem(t // nz, ny), "gz": lax.rem(t, nz)}

    barrier = pltpu.get_barrier_semaphore()

    def greet(d, c):
        pl.semaphore_signal(barrier, inc=1, device_id=dev(d)[1], device_id_type=MESH)
        return c

    lax.fori_loop(1, n, greet, 0)
    pl.semaphore_wait(barrier, n - 1)

    def copy(d):
        t, target = dev(d)
        return pltpu.make_async_remote_copy(
            src_ref=part.at[t],
            dst_ref=got.at[d],
            send_sem=send.at[d],
            recv_sem=recv.at[d],
            device_id=target,
            device_id_type=MESH,
        )

    def start(d, c):
        copy(d).start()
        return c

    lax.fori_loop(1, n, start, 0)
    out[...] = part[me]

    def take(d, c):
        copy(d).wait()
        out[...] += got[d]
        return c

    lax.fori_loop(1, n, take, 0)
    out[...] = out[...] * scale


def on_device(occupied, virtual, kernel_fields, density_grad):
    nocc, bx, by, lanes = occupied.shape
    nvir = virtual.shape[0]
    devices = lax.axis_size("gx") * lax.axis_size("gy") * lax.axis_size("gz")
    by_cell = lambda a: jnp.transpose(a, (1, 2, 0, 3))
    orb = by_cell(jnp.concatenate([occupied, virtual], axis=0))
    coefs = jnp.concatenate(
        [
            density_grad,
            kernel_fields[1:2] / 12.0,
            kernel_fields[2:4] / 144.0,
            jnp.zeros_like(density_grad[0:2]),
        ],
        axis=0,
    )
    fld = by_cell(coefs)
    k0 = kernel_fields[0][:, :, None, :]

    def slots(a):
        turned = a[::-1]
        lo = jnp.roll(turned[..., :4], 1, axis=0)
        hi = turned[..., lanes - 4:]
        return jnp.transpose(jnp.concatenate([lo, hi], axis=-1), (1, 2, 0, 3)).reshape(bx, by, -1)

    zed = jnp.stack([slots(occupied), slots(virtual)], axis=2)
    ends = jnp.concatenate([fld[..., :4], fld[..., lanes - 4:]], axis=-1)
    zfl = jnp.tile(ends, (1, 1, 1, lanes // 8))

    sds = lambda *s: jax.ShapeDtypeStruct(s, F32)
    norb = nocc + nvir
    halo_shapes = (
        sds(4, bx, by, norb, lanes),
        sds(4, 2, 2, norb, lanes),
        sds(2, 2, by, 8, lanes),
        sds(2, bx, 2, 8, lanes),
        sds(2, bx, by, 2, lanes),
        sds(2, bx, by, 8, lanes),
        sds(2, 2, 2, by, 2, lanes),
        sds(2, 2, bx, 2, 2, lanes),
    )
    vmem = pl.BlockSpec(memory_space=pltpu.VMEM)
    halos = pl.pallas_call(
        halo_kernel,
        out_shape=halo_shapes,
        in_specs=[vmem] * 4,
        out_specs=[vmem] * 8,
        scratch_shapes=[pltpu.SemaphoreType.DMA((24,)), pltpu.SemaphoreType.DMA((24,))],
        compiler_params=pltpu.CompilerParams(collective_id=0, has_side_effects=True),
        name="halo",
    )(orb, fld, zed, zfl)

    cells = bx * by * lanes
    pairs = nocc * nvir
    wide = lambda *s: pltpu.VMEM(s + (nvir, lanes), F32)
    pot, part = pl.pallas_call(
        functools.partial(main_kernel, (nocc, nvir)),
        grid=(nocc,),
        out_shape=(sds(pairs * bx * by, lanes), sds(pairs, pairs)),
        in_specs=[vmem] * 11,
        out_specs=(
            pl.BlockSpec((nvir * bx * by, lanes), lambda i: (i, 0)),
            pl.BlockSpec((pairs, pairs), lambda i: (0, 0)),
        ),
        scratch_shapes=[
            wide(bx + 8, by + 8),
            pltpu.VMEM((4, bx + 4, by + 4, nocc, lanes), F32),
            wide(4, bx + 4, by + 4),
            wide(5, bx + 4, by + 4),
            wide(bx, by),
            pltpu.VMEM((7, bx, by, 8, lanes), F32),
            pltpu.VMEM((4, 4 * by, 8, lanes), F32),
            pltpu.VMEM((4, 4 * bx, 8, lanes), F32),
            wide(bx + 4, by),
            wide(bx, by + 4),
            wide(1),
            wide(bx, by),
        ]
        + [pltpu.VMEM((pairs, cells), BF16)] * 4,
        compiler_params=pltpu.CompilerParams(
            dimension_semantics=("arbitrary",), vmem_limit_bytes=50 * 1024 * 1024
        ),
        name="response",
    )(orb, fld, k0, *halos)

    rows = pairs // devices
    casida = pl.pallas_call(
        functools.partial(scatter_kernel, 1.0 / (cells * devices)),
        out_shape=sds(rows, pairs),
        in_specs=[vmem],
        out_specs=vmem,
        scratch_shapes=[
            pltpu.VMEM((devices, rows, pairs), F32),
            pltpu.SemaphoreType.DMA((devices,)),
            pltpu.SemaphoreType.DMA((devices,)),
        ],
        compiler_params=pltpu.CompilerParams(collective_id=1, has_side_effects=True),
        name="scatter",
    )(part.reshape(devices, rows, pairs))
    return pot.reshape(pairs, bx, by, lanes), casida


def solution(mesh):
    spec = P(None, "gx", "gy", "gz")
    return jax.shard_map(
        on_device,
        mesh=mesh,
        in_specs=(spec,) * 4,
        out_specs=(spec, P(("gx", "gy", "gz"), None)),
        check_vma=False,
    )
```

```python
import functools

import jax
import jax.numpy as jnp
from jax import lax
from jax.experimental import pallas as pl
from jax.experimental.pallas import tpu as pltpu
from jax.sharding import PartitionSpec as P

MESH = pl.DeviceIdType.MESH
F32 = jnp.float32
BF16 = jnp.bfloat16


def spread(v, lane):
    lanes = v.shape[1]
    v = jnp.where((lane < 4) | (lane >= lanes - 4), v, 0.0)
    step = 8
    while step < lanes:
        v = v + pltpu.roll(v, step, 1)
        step *= 2
    return v


def slot_owner(shape):
    lane = lax.broadcasted_iota(jnp.int32, shape, 1)
    row = lax.broadcasted_iota(jnp.int32, shape, 0)
    return lax.rem(((lane + 4) // 8) + row, shape[1] // 8) == 0


def prep_kernel(cells, occ, vir, ker, grd, orb, fld, zed, zfl):
    lanes = occ.shape[1]
    nocc, nvir = occ.shape[0] // cells, vir.shape[0] // cells

    def cell(c, carry):
        for k, (ref, count, at) in enumerate(((occ, nocc, 0), (vir, nvir, nocc))):
            rows = ref[pl.ds(c, count, stride=cells), :]
            orb[c, at:at + count] = rows
            lane = lax.broadcasted_iota(jnp.int32, rows.shape, 1)
            packed = jnp.where(slot_owner(rows.shape), spread(rows, lane), 0.0)
            zed[c, k:k + 1] = jnp.sum(packed, axis=0, keepdims=True)
        g = [grd[pl.ds(k * cells + c, 1), :] for k in range(3)]
        f = [ker[pl.ds(k * cells + c, 1), :] for k in range(4)]
        rows = g + [f[1] * (1.0 / 12.0), f[2] * (1.0 / 144.0), f[3] * (1.0 / 144.0), f[0], f[0]]
        eight = jnp.concatenate(rows, axis=0)
        fld[c] = eight
        zfl[c] = spread(eight, lax.broadcasted_iota(jnp.int32, eight.shape, 1))
        return carry

    lax.fori_loop(0, cells, cell, 0)


def halo_kernel(orb, fld, zed, zfl, wide, wfld, wz, wg, send, recv, own):
    nx, ny, nz = (lax.axis_size(a) for a in ("gx", "gy", "gz"))
    x, y, z = (lax.axis_index(a) for a in ("gx", "gy", "gz"))
    bx, by = orb.shape[0], orb.shape[1]
    up = lambda v, n: lax.rem(v + 1, n)
    dn = lambda v, n: lax.rem(v + n - 1, n)
    xs = (dn(x, nx), up(x, nx))
    ys = (dn(y, ny), up(y, ny))
    zs = (dn(z, nz), up(z, nz))

    def dev(gx=None, gy=None, gz=None):
        return {
            "gx": x if gx is None else gx,
            "gy": y if gy is None else gy,
            "gz": z if gz is None else gz,
        }

    barrier = pltpu.get_barrier_semaphore()
    others = [dev(gx=v) for v in xs] + [dev(gy=v) for v in ys] + [dev(gz=v) for v in zs]
    for d in others:
        pl.semaphore_signal(barrier, inc=1, device_id=d, device_id_type=MESH)
    pl.semaphore_wait(barrier, len(others))

    copies = []

    def put(src, dst, device):
        k = len(copies)
        c = pltpu.make_async_remote_copy(
            src_ref=src,
            dst_ref=dst,
            send_sem=send.at[k],
            recv_sem=recv.at[k],
            device_id=device,
            device_id_type=MESH,
        )
        c.start()
        copies.append(c)
        return c

    def edge(b, side, width):
        return pl.ds(b - width, width) if side == 0 else pl.ds(0, width)

    def rim(b, side, width, margin):
        return pl.ds(margin - width, width) if side == 0 else pl.ds(b + margin, width)

    in_x, in_y = pl.ds(4, bx), pl.ds(4, by)
    mid_x, mid_y = pl.ds(2, bx), pl.ds(2, by)
    near = [
        put(
            orb.at[:, edge(by, side, 2)],
            wide.at[in_x, rim(by, side, 2, 4)],
            dev(gy=ys[1 - side]),
        )
        for side in range(2)
    ]
    zc = []
    for side in range(2):
        zc.append(put(zed, wz.at[side, mid_x, mid_y], dev(gz=zs[1 - side])))
        put(zfl, wg.at[side], dev(gz=zs[1 - side]))
    for side in range(2):
        put(
            orb,
            wide.at[pl.ds(0, bx) if side == 0 else pl.ds(bx + 4, bx), in_y],
            dev(gx=xs[1 - side]),
        )
        far_src = pl.ds(by - 4, 2) if side == 0 else pl.ds(2, 2)
        far_dst = pl.ds(0, 2) if side == 0 else pl.ds(by + 6, 2)
        put(orb.at[:, far_src], wide.at[in_x, far_dst], dev(gy=ys[1 - side]))
        put(
            fld.at[edge(bx, side, 2)],
            wfld.at[rim(bx, side, 2, 2), mid_y],
            dev(gx=xs[1 - side]),
        )
        put(
            fld.at[:, edge(by, side, 2)],
            wfld.at[mid_x, rim(by, side, 2, 2)],
            dev(gy=ys[1 - side]),
        )
    mine = [
        pltpu.make_async_copy(orb, wide.at[in_x, in_y], own.at[0]),
        pltpu.make_async_copy(fld, wfld.at[mid_x, mid_y], own.at[1]),
    ]
    for c in mine:
        c.start()
    for c in zc:
        c.wait_recv()
    last = []
    for side in range(2):
        own_x = pl.ds(bx, 2) if side == 0 else pl.ds(2, 2)
        own_y = pl.ds(by, 2) if side == 0 else pl.ds(2, 2)
        for k in range(2):
            last.append(
                put(
                    wz.at[k, own_x, mid_y],
                    wz.at[k, rim(bx, side, 2, 2), mid_y],
                    dev(gx=xs[1 - side]),
                )
            )
            last.append(
                put(
                    wz.at[k, mid_x, own_y],
                    wz.at[k, mid_x, rim(by, side, 2, 2)],
                    dev(gy=ys[1 - side]),
                )
            )
    for sy in range(2):
        near[sy].wait_recv()
        for sx in range(2):
            own_x = pl.ds(bx + 2, 2) if sx == 0 else pl.ds(4, 2)
            rim_y = rim(by, sy, 2, 4)
            put(
                wide.at[own_x, rim_y],
                wide.at[rim(bx, sx, 2, 4), rim_y],
                dev(gx=xs[1 - sx]),
            )
    early = near + zc
    for c in early:
        c.wait_send()
    for c in copies:
        if not any(c is e for e in early):
            c.wait()
    for c in mine:
        c.wait()


def main_kernel(
    norb, wide, wfld, wz, wg,
    pot, part,
    nS, oS, vS, vE, eF, C, A0, A1, f0, f1, f2, base, ph, plo, nh, nl,
):
    nocc, nvir = norb
    bx, by = wide.shape[0] - 8, wide.shape[1] - 8
    lanes = wide.shape[3]
    i = pl.program_id(0)
    shifts = (1, -1, 2, -2)

    center = [(x, y) for x in range(bx) for y in range(by)]
    xarm = [(x, y) for x in (-2, -1, bx, bx + 1) for y in range(by)]
    yarm = [(x, y) for x in range(bx) for y in (-2, -1, by, by + 1)]
    near = center + xarm + yarm
    far = [(x, y) for x in (-4, -3, bx + 2, bx + 3) for y in range(by)]
    far += [(x, y) for x in range(bx) for y in (-4, -3, by + 2, by + 3)]
    far += [(x, y) for x in (-2, -1, bx, bx + 1) for y in (-2, -1, by, by + 1)]
    lane = lax.broadcasted_iota(jnp.int32, (nvir, lanes), 1)

    def slope(f):
        return 8.0 * (f(1) - f(-1)) - (f(2) - f(-2))

    @pl.when(i == 0)
    def _():
        lane1 = lax.broadcasted_iota(jnp.int32, (1, lanes), 1)
        upper = (lane1 & 7) < 4
        owner = slot_owner((nocc, lanes))

        def wrapped(s):
            return lane < s if s > 0 else lane >= lanes + s

        def pair(x, y):
            rows = jnp.where(upper, wz[1, x, y], wz[0, x, y])
            alt = [
                pltpu.roll(
                    jnp.broadcast_to(rows[k:k + 1], (n, lanes)), 0, 1, stride=8, stride_axis=0
                )
                for k, n in enumerate((nocc, nvir))
            ]
            return rows, alt, wide[x + 2, y + 2, 0:nocc], wide[x + 2, y + 2, nocc:nocc + nvir]

        def prepare(x, y):
            rows, (o_alt, v_alt), o_own, v_own = pair(x, y)
            vE[0, x, y] = rows[0:1] * spread(v_alt, lane)
            for k, s in enumerate(shifts):
                m = wrapped(s)
                roll = (-s) % lanes
                scale = 8.0 if abs(s) == 1 else 1.0
                oS[k, x, y] = scale * pltpu.roll(jnp.where(m, o_alt, o_own), roll, 1)
                vS[k, x, y] = pltpu.roll(jnp.where(m, v_alt, v_own), roll, 1)

        def band(t, c):
            prepare(t // by, 2 + lax.rem(t, by))
            return c

        lax.fori_loop(0, (bx + 4) * by, band, 0)

        def sides(t, c):
            y = lax.rem(t, 4)
            prepare(2 + t // 4, jnp.where(y < 2, y, y + by))
            return c

        lax.fori_loop(0, bx * 4, sides, 0)

        def flux_at(me, f, s, n):
            g = [f[k:k + 1] for k in range(3)]
            total = (f[3:4] * g[me]) * n
            for k in range(3):
                c = f[4:5] * g[me] * g[k]
                total += (c + f[5:6] if k == me else c) * s[k]
            return total

        def edges(t, carry):
            x, y = t // by + 2, lax.rem(t, by) + 2
            rows, (o_alt, v_alt), o_own, v_own = pair(x, y)
            p = []
            for k, s in enumerate(shifts):
                m = wrapped(s)
                roll = (-s) % lanes
                oe = spread(pltpu.roll(jnp.where(m, o_own, o_alt), roll, 1), lane)
                ve = spread(pltpu.roll(jnp.where(m, v_own, v_alt), roll, 1), lane)
                oe = jnp.sum(jnp.where(owner, oe, 0.0), axis=0, keepdims=True)
                p.append(oe * ve)
            s2 = 8.0 * (p[0] - p[1]) - (p[2] - p[3])
            s0 = slope(lambda d: vE[0, x + d, y])
            s1 = slope(lambda d: vE[0, x, y + d])
            g = jnp.where(upper, wg[1, x - 2, y - 2], wg[0, x - 2, y - 2])
            eF[x - 2, y - 2] = flux_at(2, g, (s0, s1, s2), vE[0, x, y])
            f = wfld[x, y]
            for k in range(7):
                C[k, x - 2, y - 2] = jnp.broadcast_to(f[k:k + 1], (8, lanes))
            return carry

        lax.fori_loop(0, bx * by, edges, 0)

        def arm_coefs(arm, at, me, f):
            gm = f[me:me + 1]
            for k in range(3):
                c = f[4:5] * gm * f[k:k + 1]
                if k == me:
                    c = c + f[5:6]
                arm[k, at] = jnp.broadcast_to(c, (8, lanes))
            arm[3, at] = jnp.broadcast_to(f[3:4] * gm, (8, lanes))

        def arm_x(t, c):
            x = t // by
            arm_coefs(A0, t, 0, wfld[jnp.where(x < 2, x, x + bx), 2 + lax.rem(t, by)])
            return c

        lax.fori_loop(0, 4 * by, arm_x, 0)

        def arm_y(t, c):
            y = lax.rem(t, 4)
            arm_coefs(A1, t, 1, wfld[2 + t // 4, jnp.where(y < 2, y, y + by)])
            return c

        lax.fori_loop(0, 4 * bx, arm_y, 0)

    def rows2(c):
        return jnp.concatenate([c] * (nvir // 8), axis=0)

    off = 4
    for x, y in near + far:
        cell = wide.at[x + off, y + off]
        nS[x + off, y + off] = cell[pl.ds(i, 1)] * cell[nocc:nocc + nvir]

    def n_at(x, y):
        return nS[x + off, y + off]

    def slopes(x, y):
        s0 = slope(lambda t: n_at(x + t, y))
        s1 = slope(lambda t: n_at(x, y + t))
        p = [oS[k, x + 2, y + 2, pl.ds(i, 1)] * vS[k, x + 2, y + 2] for k in range(4)]
        return s0, s1, (p[0] - p[1]) - (p[2] - p[3])

    for arm, cells, out in ((A0, xarm, f0), (A1, yarm, f1)):
        for at, (x, y) in enumerate(cells):
            s0, s1, s2 = slopes(x, y)
            value = (
                rows2(arm[0, at]) * s0
                + rows2(arm[1, at]) * s1
                + rows2(arm[2, at]) * s2
                + rows2(arm[3, at]) * n_at(x, y)
            )
            if out is f0:
                f0[x + 2, y] = value
            else:
                f1[x, y + 2] = value

    back = 8 * i
    row0 = pl.multiple_of(i * nvir, nvir)
    for x, y in center:
        s0, s1, s2 = slopes(x, y)
        g0, g1, g2, k1, k2, k3, kk = (rows2(C[k, x, y]) for k in range(7))
        n = n_at(x, y)
        al = g0 * s0 + g1 * s1 + g2 * s2
        sc = k1 * n + k2 * al
        f0[x + 2, y] = sc * g0 + k3 * s0
        f1[x, y + 2] = sc * g1 + k3 * s1
        f = sc * g2 + k3 * s2
        e = pltpu.roll(eF[x, y], back, 1)
        up1 = pltpu.roll(jnp.where(lane < 1, e, f), lanes - 1, 1)
        up2 = pltpu.roll(jnp.where(lane < 2, e, f), lanes - 2, 1)
        dn1 = pltpu.roll(jnp.where(lane >= lanes - 1, e, f), 1, 1)
        dn2 = pltpu.roll(jnp.where(lane >= lanes - 2, e, f), 2, 1)
        base[x, y] = kk * n + k1 * al - (8.0 * (up1 - dn1) - (up2 - dn2))
        at = (x * by + y) * lanes
        hi = n.astype(BF16)
        nh[pl.ds(row0, nvir), at:at + lanes] = hi
        nl[pl.ds(row0, nvir), at:at + lanes] = (n - hi.astype(F32)).astype(BF16)

    for x, y in center:
        inner = (f0[x + 3, y] - f0[x + 1, y]) + (f1[x, y + 3] - f1[x, y + 1])
        outer = (f0[x + 4, y] - f0[x, y]) + (f1[x, y + 4] - f1[x, y])
        v = base[x, y] - (8.0 * inner - outer)
        cell = x * by + y
        pot[pl.ds(cell, nvir, stride=bx * by), :] = v
        at = cell * lanes
        hi = v.astype(BF16)
        ph[pl.ds(row0, nvir), at:at + lanes] = hi
        plo[pl.ds(row0, nvir), at:at + lanes] = (v - hi.astype(F32)).astype(BF16)

    @pl.when(i == nocc - 1)
    def _():
        def dot(a, b):
            return lax.dot_general(
                a[...], b[...], (((1,), (1,)), ((), ())), preferred_element_type=F32
            )

        part[...] = dot(nh, ph) + dot(nh, plo) + dot(nl, ph)


def scatter_kernel(scale, part, out, got, send, recv):
    nx, ny, nz = (lax.axis_size(a) for a in ("gx", "gy", "gz"))
    n = nx * ny * nz
    me = (lax.axis_index("gx") * ny + lax.axis_index("gy")) * nz + lax.axis_index("gz")

    def dev(d):
        t = lax.rem(me + d, n)
        return t, {"gx": t // (ny * nz), "gy": lax.rem(t // nz, ny), "gz": lax.rem(t, nz)}

    barrier = pltpu.get_barrier_semaphore()

    def greet(d, c):
        pl.semaphore_signal(barrier, inc=1, device_id=dev(d)[1], device_id_type=MESH)
        return c

    lax.fori_loop(1, n, greet, 0)
    pl.semaphore_wait(barrier, n - 1)

    def copy(d):
        t, target = dev(d)
        return pltpu.make_async_remote_copy(
            src_ref=part.at[t],
            dst_ref=got.at[d],
            send_sem=send.at[d],
            recv_sem=recv.at[d],
            device_id=target,
            device_id_type=MESH,
        )

    def start(d, c):
        copy(d).start()
        return c

    lax.fori_loop(1, n, start, 0)
    out[...] = part[me]

    def take(d, c):
        copy(d).wait()
        out[...] += got[d]
        return c

    lax.fori_loop(1, n, take, 0)
    out[...] = out[...] * scale


def on_device(occupied, virtual, kernel_fields, density_grad):
    nocc, bx, by, lanes = occupied.shape
    nvir = virtual.shape[0]
    devices = lax.axis_size("gx") * lax.axis_size("gy") * lax.axis_size("gz")
    sds = lambda *s: jax.ShapeDtypeStruct(s, F32)
    norb = nocc + nvir
    vmem = pl.BlockSpec(memory_space=pltpu.VMEM)
    plane = bx * by
    flat = lambda a: a.reshape(-1, lanes)
    orb, fld, zed, zfl = pl.pallas_call(
        functools.partial(prep_kernel, plane),
        out_shape=(
            sds(plane, norb, lanes),
            sds(plane, 8, lanes),
            sds(plane, 2, lanes),
            sds(plane, 8, lanes),
        ),
        in_specs=[vmem] * 4,
        out_specs=[vmem] * 4,
        name="prep",
    )(flat(occupied), flat(virtual), flat(kernel_fields), flat(density_grad))
    by_cell = lambda a: a.reshape((bx, by) + a.shape[1:])

    halos = pl.pallas_call(
        halo_kernel,
        out_shape=(
            sds(bx + 8, by + 8, norb, lanes),
            sds(bx + 4, by + 4, 8, lanes),
            sds(2, bx + 4, by + 4, 2, lanes),
            sds(2, bx, by, 8, lanes),
        ),
        in_specs=[vmem] * 4,
        out_specs=[vmem] * 4,
        scratch_shapes=[
            pltpu.SemaphoreType.DMA((26,)),
            pltpu.SemaphoreType.DMA((26,)),
            pltpu.SemaphoreType.DMA((2,)),
        ],
        compiler_params=pltpu.CompilerParams(collective_id=0, has_side_effects=True),
        name="halo",
    )(by_cell(orb), by_cell(fld), by_cell(zed), by_cell(zfl))

    cells = bx * by * lanes
    pairs = nocc * nvir
    wide = lambda *s: pltpu.VMEM(s + (nvir, lanes), F32)
    pot, part = pl.pallas_call(
        functools.partial(main_kernel, (nocc, nvir)),
        grid=(nocc,),
        out_shape=(sds(pairs * bx * by, lanes), sds(pairs, pairs)),
        in_specs=[vmem] * 4,
        out_specs=(
            pl.BlockSpec((nvir * bx * by, lanes), lambda i: (i, 0)),
            pl.BlockSpec((pairs, pairs), lambda i: (0, 0)),
        ),
        scratch_shapes=[
            wide(bx + 8, by + 8),
            pltpu.VMEM((4, bx + 4, by + 4, nocc, lanes), F32),
            wide(4, bx + 4, by + 4),
            wide(1, bx + 4, by + 4),
            wide(bx, by),
            pltpu.VMEM((7, bx, by, 8, lanes), F32),
            pltpu.VMEM((4, 4 * by, 8, lanes), F32),
            pltpu.VMEM((4, 4 * bx, 8, lanes), F32),
            wide(bx + 4, by),
            wide(bx, by + 4),
            wide(1),
            wide(bx, by),
        ]
        + [pltpu.VMEM((pairs, cells), BF16)] * 4,
        compiler_params=pltpu.CompilerParams(
            dimension_semantics=("arbitrary",), vmem_limit_bytes=50 * 1024 * 1024
        ),
        name="response",
    )(*halos)

    rows = pairs // devices
    casida = pl.pallas_call(
        functools.partial(scatter_kernel, 1.0 / (cells * devices)),
        out_shape=sds(rows, pairs),
        in_specs=[vmem],
        out_specs=vmem,
        scratch_shapes=[
            pltpu.VMEM((devices, rows, pairs), F32),
            pltpu.SemaphoreType.DMA((devices,)),
            pltpu.SemaphoreType.DMA((devices,)),
        ],
        compiler_params=pltpu.CompilerParams(collective_id=1, has_side_effects=True),
        name="scatter",
    )(part.reshape(devices, rows, pairs))
    return pot.reshape(pairs, bx, by, lanes), casida


def solution(mesh):
    spec = P(None, "gx", "gy", "gz")
    return jax.shard_map(
        on_device,
        mesh=mesh,
        in_specs=(spec,) * 4,
        out_specs=(spec, P(("gx", "gy", "gz"), None)),
        check_vma=False,
    )
```

```python
import functools

import jax
import jax.numpy as jnp
from jax import lax
from jax.experimental import pallas as pl
from jax.experimental.pallas import tpu as pltpu
from jax.sharding import PartitionSpec as P

MESH = pl.DeviceIdType.MESH
F32 = jnp.float32
BF16 = jnp.bfloat16


def spread(v, lane):
    lanes = v.shape[1]
    v = jnp.where((lane < 4) | (lane >= lanes - 4), v, 0.0)
    step = 8
    while step < lanes:
        turns = [pltpu.roll(v, k * step, 1) for k in range(1, 4) if k * step < lanes]
        for t in turns:
            v = v + t
        step *= 4
    return v


def slot_owner(shape):
    lane = lax.broadcasted_iota(jnp.int32, shape, 1)
    row = lax.broadcasted_iota(jnp.int32, shape, 0)
    return lax.rem(((lane + 4) // 8) + row, shape[1] // 8) == 0


def prep_kernel(cells, occ, vir, ker, grd, orb, fld, zed, zfl):
    lanes = occ.shape[1]
    nocc, nvir = occ.shape[0] // cells, vir.shape[0] // cells

    def cell(c, carry):
        for k, (ref, count, at) in enumerate(((occ, nocc, 0), (vir, nvir, nocc))):
            rows = ref[pl.ds(c, count, stride=cells), :]
            orb[c, at:at + count] = rows
            lane = lax.broadcasted_iota(jnp.int32, rows.shape, 1)
            packed = jnp.where(slot_owner(rows.shape), spread(rows, lane), 0.0)
            zed[c, k:k + 1] = jnp.sum(packed, axis=0, keepdims=True)
        g = [grd[pl.ds(k * cells + c, 1), :] for k in range(3)]
        f = [ker[pl.ds(k * cells + c, 1), :] for k in range(4)]
        rows = g + [f[1] * (1.0 / 12.0), f[2] * (1.0 / 144.0), f[3] * (1.0 / 144.0), f[0], f[0]]
        eight = jnp.concatenate(rows, axis=0)
        fld[c] = eight
        zfl[c] = spread(eight, lax.broadcasted_iota(jnp.int32, eight.shape, 1))
        return carry

    lax.fori_loop(0, cells, cell, 0, unroll=4)


def halo_kernel(orb, fld, zed, zfl, wide, wfld, wz, wg, send, recv, own):
    nx, ny, nz = (lax.axis_size(a) for a in ("gx", "gy", "gz"))
    x, y, z = (lax.axis_index(a) for a in ("gx", "gy", "gz"))
    bx, by = orb.shape[0], orb.shape[1]
    up = lambda v, n: lax.rem(v + 1, n)
    dn = lambda v, n: lax.rem(v + n - 1, n)
    xs = (dn(x, nx), up(x, nx))
    ys = (dn(y, ny), up(y, ny))
    zs = (dn(z, nz), up(z, nz))

    def dev(gx=None, gy=None, gz=None):
        return {
            "gx": x if gx is None else gx,
            "gy": y if gy is None else gy,
            "gz": z if gz is None else gz,
        }

    barrier = pltpu.get_barrier_semaphore()
    others = [dev(gx=v) for v in xs] + [dev(gy=v) for v in ys] + [dev(gz=v) for v in zs]
    for d in others:
        pl.semaphore_signal(barrier, inc=1, device_id=d, device_id_type=MESH)
    pl.semaphore_wait(barrier, len(others))

    copies = []

    def put(src, dst, device):
        k = len(copies)
        c = pltpu.make_async_remote_copy(
            src_ref=src,
            dst_ref=dst,
            send_sem=send.at[k],
            recv_sem=recv.at[k],
            device_id=device,
            device_id_type=MESH,
        )
        c.start()
        copies.append(c)
        return c

    def edge(b, side, width):
        return pl.ds(b - width, width) if side == 0 else pl.ds(0, width)

    def rim(b, side, width, margin):
        return pl.ds(margin - width, width) if side == 0 else pl.ds(b + margin, width)

    in_x, in_y = pl.ds(4, bx), pl.ds(4, by)
    mid_x, mid_y = pl.ds(2, bx), pl.ds(2, by)
    near = [
        put(
            orb.at[:, edge(by, side, 2)],
            wide.at[in_x, rim(by, side, 2, 4)],
            dev(gy=ys[1 - side]),
        )
        for side in range(2)
    ]
    zc = []
    for side in range(2):
        zc.append(put(zed, wz.at[side, mid_x, mid_y], dev(gz=zs[1 - side])))
        put(zfl, wg.at[side], dev(gz=zs[1 - side]))
    for side in range(2):
        put(
            orb,
            wide.at[pl.ds(0, bx) if side == 0 else pl.ds(bx + 4, bx), in_y],
            dev(gx=xs[1 - side]),
        )
        far_src = pl.ds(by - 4, 2) if side == 0 else pl.ds(2, 2)
        far_dst = pl.ds(0, 2) if side == 0 else pl.ds(by + 6, 2)
        put(orb.at[:, far_src], wide.at[in_x, far_dst], dev(gy=ys[1 - side]))
        put(
            fld.at[edge(bx, side, 2)],
            wfld.at[rim(bx, side, 2, 2), mid_y],
            dev(gx=xs[1 - side]),
        )
        put(
            fld.at[:, edge(by, side, 2)],
            wfld.at[mid_x, rim(by, side, 2, 2)],
            dev(gy=ys[1 - side]),
        )
    mine = [
        pltpu.make_async_copy(orb, wide.at[in_x, in_y], own.at[0]),
        pltpu.make_async_copy(fld, wfld.at[mid_x, mid_y], own.at[1]),
    ]
    for c in mine:
        c.start()
    for c in zc:
        c.wait_recv()
    last = []
    for side in range(2):
        own_x = pl.ds(bx, 2) if side == 0 else pl.ds(2, 2)
        own_y = pl.ds(by, 2) if side == 0 else pl.ds(2, 2)
        for k in range(2):
            last.append(
                put(
                    wz.at[k, own_x, mid_y],
                    wz.at[k, rim(bx, side, 2, 2), mid_y],
                    dev(gx=xs[1 - side]),
                )
            )
            last.append(
                put(
                    wz.at[k, mid_x, own_y],
                    wz.at[k, mid_x, rim(by, side, 2, 2)],
                    dev(gy=ys[1 - side]),
                )
            )
    for sy in range(2):
        near[sy].wait_recv()
        for sx in range(2):
            own_x = pl.ds(bx + 2, 2) if sx == 0 else pl.ds(4, 2)
            rim_y = rim(by, sy, 2, 4)
            put(
                wide.at[own_x, rim_y],
                wide.at[rim(bx, sx, 2, 4), rim_y],
                dev(gx=xs[1 - sx]),
            )
    early = near + zc
    for c in early:
        c.wait_send()
    for c in copies:
        if not any(c is e for e in early):
            c.wait()
    for c in mine:
        c.wait()


def main_kernel(
    norb, wide, wfld, wz, wg,
    pot, part,
    nS, oS, vS, vE, eF, C, A0, A1, f0, f1, f2, base, ph, plo, nh, nl,
):
    nocc, nvir = norb
    bx, by = wide.shape[0] - 8, wide.shape[1] - 8
    lanes = wide.shape[3]
    i = pl.program_id(0)
    shifts = (1, -1, 2, -2)

    center = [(x, y) for x in range(bx) for y in range(by)]
    xarm = [(x, y) for x in (-2, -1, bx, bx + 1) for y in range(by)]
    yarm = [(x, y) for x in range(bx) for y in (-2, -1, by, by + 1)]
    near = center + xarm + yarm
    far = [(x, y) for x in (-4, -3, bx + 2, bx + 3) for y in range(by)]
    far += [(x, y) for x in range(bx) for y in (-4, -3, by + 2, by + 3)]
    far += [(x, y) for x in (-2, -1, bx, bx + 1) for y in (-2, -1, by, by + 1)]
    lane = lax.broadcasted_iota(jnp.int32, (nvir, lanes), 1)

    def slope(f):
        return 8.0 * (f(1) - f(-1)) - (f(2) - f(-2))

    @pl.when(i == 0)
    def _():
        lane1 = lax.broadcasted_iota(jnp.int32, (1, lanes), 1)
        upper = (lane1 & 7) < 4
        owner = slot_owner((nocc, lanes))

        def wrapped(s):
            return lane < s if s > 0 else lane >= lanes + s

        def pair(x, y):
            rows = jnp.where(upper, wz[1, x, y], wz[0, x, y])
            alt = [
                pltpu.roll(
                    jnp.broadcast_to(rows[k:k + 1], (n, lanes)), 0, 1, stride=8, stride_axis=0
                )
                for k, n in enumerate((nocc, nvir))
            ]
            return rows, alt, wide[x + 2, y + 2, 0:nocc], wide[x + 2, y + 2, nocc:nocc + nvir]

        def prepare(x, y):
            rows, (o_alt, v_alt), o_own, v_own = pair(x, y)
            vE[0, x, y] = rows[0:1] * spread(v_alt, lane)
            for k, s in enumerate(shifts):
                m = wrapped(s)
                roll = (-s) % lanes
                scale = 8.0 if abs(s) == 1 else 1.0
                oS[k, x, y] = scale * pltpu.roll(jnp.where(m, o_alt, o_own), roll, 1)
                vS[k, x, y] = pltpu.roll(jnp.where(m, v_alt, v_own), roll, 1)

        def band(t, c):
            prepare(t // by, 2 + lax.rem(t, by))
            return c

        lax.fori_loop(0, (bx + 4) * by, band, 0, unroll=4)

        def sides(t, c):
            y = lax.rem(t, 4)
            prepare(2 + t // 4, jnp.where(y < 2, y, y + by))
            return c

        lax.fori_loop(0, bx * 4, sides, 0, unroll=4)

        def flux_at(me, f, s, n):
            g = [f[k:k + 1] for k in range(3)]
            total = (f[3:4] * g[me]) * n
            for k in range(3):
                c = f[4:5] * g[me] * g[k]
                total += (c + f[5:6] if k == me else c) * s[k]
            return total

        def edges(t, carry):
            x, y = t // by + 2, lax.rem(t, by) + 2
            rows, (o_alt, v_alt), o_own, v_own = pair(x, y)
            p = []
            for k, s in enumerate(shifts):
                m = wrapped(s)
                roll = (-s) % lanes
                oe = spread(pltpu.roll(jnp.where(m, o_own, o_alt), roll, 1), lane)
                ve = spread(pltpu.roll(jnp.where(m, v_own, v_alt), roll, 1), lane)
                oe = jnp.sum(jnp.where(owner, oe, 0.0), axis=0, keepdims=True)
                p.append(oe * ve)
            s2 = 8.0 * (p[0] - p[1]) - (p[2] - p[3])
            s0 = slope(lambda d: vE[0, x + d, y])
            s1 = slope(lambda d: vE[0, x, y + d])
            g = jnp.where(upper, wg[1, x - 2, y - 2], wg[0, x - 2, y - 2])
            eF[x - 2, y - 2] = flux_at(2, g, (s0, s1, s2), vE[0, x, y])
            f = wfld[x, y]
            for k in range(7):
                C[k, x - 2, y - 2] = jnp.broadcast_to(f[k:k + 1], (8, lanes))
            return carry

        lax.fori_loop(0, bx * by, edges, 0, unroll=4)

        def arm_coefs(arm, at, me, f):
            gm = f[me:me + 1]
            for k in range(3):
                c = f[4:5] * gm * f[k:k + 1]
                if k == me:
                    c = c + f[5:6]
                arm[k, at] = jnp.broadcast_to(c, (8, lanes))
            arm[3, at] = jnp.broadcast_to(f[3:4] * gm, (8, lanes))

        def arm_x(t, c):
            x = t // by
            arm_coefs(A0, t, 0, wfld[jnp.where(x < 2, x, x + bx), 2 + lax.rem(t, by)])
            return c

        lax.fori_loop(0, 4 * by, arm_x, 0, unroll=4)

        def arm_y(t, c):
            y = lax.rem(t, 4)
            arm_coefs(A1, t, 1, wfld[2 + t // 4, jnp.where(y < 2, y, y + by)])
            return c

        lax.fori_loop(0, 4 * bx, arm_y, 0, unroll=4)

    def rows2(c):
        return jnp.concatenate([c] * (nvir // 8), axis=0)

    off = 4
    for x, y in near + far:
        cell = wide.at[x + off, y + off]
        nS[x + off, y + off] = cell[pl.ds(i, 1)] * cell[nocc:nocc + nvir]

    def n_at(x, y):
        return nS[x + off, y + off]

    def slopes(x, y):
        s0 = slope(lambda t: n_at(x + t, y))
        s1 = slope(lambda t: n_at(x, y + t))
        p = [oS[k, x + 2, y + 2, pl.ds(i, 1)] * vS[k, x + 2, y + 2] for k in range(4)]
        return s0, s1, (p[0] - p[1]) - (p[2] - p[3])

    for arm, cells, out in ((A0, xarm, f0), (A1, yarm, f1)):
        for at, (x, y) in enumerate(cells):
            s0, s1, s2 = slopes(x, y)
            value = (
                rows2(arm[0, at]) * s0
                + rows2(arm[1, at]) * s1
                + rows2(arm[2, at]) * s2
                + rows2(arm[3, at]) * n_at(x, y)
            )
            if out is f0:
                f0[x + 2, y] = value
            else:
                f1[x, y + 2] = value

    back = 8 * i
    row0 = pl.multiple_of(i * nvir, nvir)
    for x, y in center:
        s0, s1, s2 = slopes(x, y)
        g0, g1, g2, k1, k2, k3, kk = (rows2(C[k, x, y]) for k in range(7))
        n = n_at(x, y)
        al = g0 * s0 + g1 * s1 + g2 * s2
        sc = k1 * n + k2 * al
        f0[x + 2, y] = sc * g0 + k3 * s0
        f1[x, y + 2] = sc * g1 + k3 * s1
        f = sc * g2 + k3 * s2
        e = pltpu.roll(eF[x, y], back, 1)
        up1 = pltpu.roll(jnp.where(lane < 1, e, f), lanes - 1, 1)
        up2 = pltpu.roll(jnp.where(lane < 2, e, f), lanes - 2, 1)
        dn1 = pltpu.roll(jnp.where(lane >= lanes - 1, e, f), 1, 1)
        dn2 = pltpu.roll(jnp.where(lane >= lanes - 2, e, f), 2, 1)
        base[x, y] = kk * n + k1 * al - (8.0 * (up1 - dn1) - (up2 - dn2))
        at = (x * by + y) * lanes
        hi = n.astype(BF16)
        nh[pl.ds(row0, nvir), at:at + lanes] = hi
        nl[pl.ds(row0, nvir), at:at + lanes] = (n - hi.astype(F32)).astype(BF16)

    for x, y in center:
        inner = (f0[x + 3, y] - f0[x + 1, y]) + (f1[x, y + 3] - f1[x, y + 1])
        outer = (f0[x + 4, y] - f0[x, y]) + (f1[x, y + 4] - f1[x, y])
        v = base[x, y] - (8.0 * inner - outer)
        cell = x * by + y
        pot[pl.ds(cell, nvir, stride=bx * by), :] = v
        at = cell * lanes
        hi = v.astype(BF16)
        ph[pl.ds(row0, nvir), at:at + lanes] = hi
        plo[pl.ds(row0, nvir), at:at + lanes] = (v - hi.astype(F32)).astype(BF16)

    @pl.when(i == nocc - 1)
    def _():
        def dot(a, b):
            return lax.dot_general(
                a[...], b[...], (((1,), (1,)), ((), ())), preferred_element_type=F32
            )

        part[...] = dot(nh, ph) + dot(nh, plo) + dot(nl, ph)


def scatter_kernel(scale, part, out, got, acc, got2, send, recv, send2, recv2):
    nx, ny, nz = (lax.axis_size(a) for a in ("gx", "gy", "gz"))
    x, y, z = (lax.axis_index(a) for a in ("gx", "gy", "gz"))
    n = nx * nz
    me = x * nz + z

    def plane(d):
        t = lax.rem(me + d, n)
        tx, tz = t // nz, lax.rem(t, nz)
        return tx, tz, {"gx": tx, "gy": y, "gz": tz}

    def column(d):
        t = lax.rem(y + d, ny)
        return t, {"gx": x, "gy": t, "gz": z}

    barrier = pltpu.get_barrier_semaphore()
    for d in range(1, n):
        pl.semaphore_signal(barrier, inc=1, device_id=plane(d)[2], device_id_type=MESH)
    for d in range(1, ny):
        pl.semaphore_signal(barrier, inc=1, device_id=column(d)[1], device_id_type=MESH)
    pl.semaphore_wait(barrier, n - 1 + ny - 1)

    first = []
    for d in range(1, n):
        tx, tz, target = plane(d)
        c = pltpu.make_async_remote_copy(
            src_ref=part.at[tx, :, tz],
            dst_ref=got.at[d],
            send_sem=send.at[d],
            recv_sem=recv.at[d],
            device_id=target,
            device_id_type=MESH,
        )
        c.start()
        first.append(c)
    total = part[x, :, z]
    for d, c in enumerate(first):
        c.wait_recv()
        total = total + got[d + 1]
    acc[...] = total
    second = []
    for d in range(1, ny):
        t, target = column(d)
        c = pltpu.make_async_remote_copy(
            src_ref=acc.at[t],
            dst_ref=got2.at[d],
            send_sem=send2.at[d],
            recv_sem=recv2.at[d],
            device_id=target,
            device_id_type=MESH,
        )
        c.start()
        second.append(c)
    for c in first:
        c.wait_send()
    total = acc[y]
    for d, c in enumerate(second):
        c.wait()
        total = total + got2[d + 1]
    out[...] = total * scale


def on_device(occupied, virtual, kernel_fields, density_grad):
    nocc, bx, by, lanes = occupied.shape
    nvir = virtual.shape[0]
    nx, ny, nz = (lax.axis_size(a) for a in ("gx", "gy", "gz"))
    devices = nx * ny * nz
    sds = lambda *s: jax.ShapeDtypeStruct(s, F32)
    norb = nocc + nvir
    vmem = pl.BlockSpec(memory_space=pltpu.VMEM)
    plane = bx * by
    flat = lambda a: a.reshape(-1, lanes)
    orb, fld, zed, zfl = pl.pallas_call(
        functools.partial(prep_kernel, plane),
        out_shape=(
            sds(plane, norb, lanes),
            sds(plane, 8, lanes),
            sds(plane, 2, lanes),
            sds(plane, 8, lanes),
        ),
        in_specs=[vmem] * 4,
        out_specs=[vmem] * 4,
        compiler_params=pltpu.CompilerParams(vmem_limit_bytes=8 * 1024 * 1024),
        name="prep",
    )(flat(occupied), flat(virtual), flat(kernel_fields), flat(density_grad))
    by_cell = lambda a: a.reshape((bx, by) + a.shape[1:])

    halos = pl.pallas_call(
        halo_kernel,
        out_shape=(
            sds(bx + 8, by + 8, norb, lanes),
            sds(bx + 4, by + 4, 8, lanes),
            sds(2, bx + 4, by + 4, 2, lanes),
            sds(2, bx, by, 8, lanes),
        ),
        in_specs=[pl.BlockSpec(memory_space=pl.ANY)] * 4,
        out_specs=[pl.BlockSpec(memory_space=pl.ANY)] * 4,
        scratch_shapes=[
            pltpu.SemaphoreType.DMA((26,)),
            pltpu.SemaphoreType.DMA((26,)),
            pltpu.SemaphoreType.DMA((2,)),
        ],
        compiler_params=pltpu.CompilerParams(
            collective_id=0, has_side_effects=True, vmem_limit_bytes=8 * 1024 * 1024
        ),
        name="halo",
    )(by_cell(orb), by_cell(fld), by_cell(zed), by_cell(zfl))

    cells = bx * by * lanes
    pairs = nocc * nvir
    wide = lambda *s: pltpu.VMEM(s + (nvir, lanes), F32)
    pot, part = pl.pallas_call(
        functools.partial(main_kernel, (nocc, nvir)),
        grid=(nocc,),
        out_shape=(sds(pairs * bx * by, lanes), sds(pairs, pairs)),
        in_specs=[vmem] * 4,
        out_specs=(
            pl.BlockSpec((nvir * bx * by, lanes), lambda i: (i, 0)),
            pl.BlockSpec((pairs, pairs), lambda i: (0, 0)),
        ),
        scratch_shapes=[
            wide(bx + 8, by + 8),
            pltpu.VMEM((4, bx + 4, by + 4, nocc, lanes), F32),
            wide(4, bx + 4, by + 4),
            wide(1, bx + 4, by + 4),
            wide(bx, by),
            pltpu.VMEM((7, bx, by, 8, lanes), F32),
            pltpu.VMEM((4, 4 * by, 8, lanes), F32),
            pltpu.VMEM((4, 4 * bx, 8, lanes), F32),
            wide(bx + 4, by),
            wide(bx, by + 4),
            wide(1),
            wide(bx, by),
        ]
        + [pltpu.VMEM((pairs, cells), BF16)] * 4,
        compiler_params=pltpu.CompilerParams(
            dimension_semantics=("arbitrary",), vmem_limit_bytes=28 * 1024 * 1024
        ),
        name="response",
    )(*halos)

    rows = pairs // devices
    casida = pl.pallas_call(
        functools.partial(scatter_kernel, 1.0 / (cells * devices)),
        out_shape=sds(rows, pairs),
        in_specs=[vmem],
        out_specs=vmem,
        scratch_shapes=[
            pltpu.VMEM((nx * nz, ny, rows, pairs), F32),
            pltpu.VMEM((ny, rows, pairs), F32),
            pltpu.VMEM((ny, rows, pairs), F32),
            pltpu.SemaphoreType.DMA((nx * nz,)),
            pltpu.SemaphoreType.DMA((nx * nz,)),
            pltpu.SemaphoreType.DMA((ny,)),
            pltpu.SemaphoreType.DMA((ny,)),
        ],
        compiler_params=pltpu.CompilerParams(collective_id=1, has_side_effects=True),
        name="scatter",
    )(part.reshape(nx, ny, nz, rows, pairs))
    return pot.reshape(pairs, bx, by, lanes), casida


def solution(mesh):
    spec = P(None, "gx", "gy", "gz")
    return jax.shard_map(
        on_device,
        mesh=mesh,
        in_specs=(spec,) * 4,
        out_specs=(spec, P(("gx", "gy", "gz"), None)),
        check_vma=False,
    )
```
